256 devices in a mesh: fine: 32 (over z, x_lo, core), coarse: 8 (over y, x_hi).
Axes of the slice: x: 4 (x_hi: 2, x_lo: 2; x = x_hi * 2 + x_lo), y: 4, z: 8, core: 2. Of those that a mesh axis runs over, the one named last changes fastest.
Arguments:
- start_states: float32 [32, 1, 64, 64, 256], P('fine', None, 'coarse'), may hold values from -6 to 6
- weights: bfloat16 [128, 9, 256, 256], P('fine'), may hold values from -0.125 to 0.125
- biases: float32 [128, 256], P('fine'), may hold values from -3 to 3
- step_sizes: float32 [128], P('fine'), may hold values from 0.1 to 0.4
Outputs:
- corrected: float32 [32, 1, 64, 64, 256], P('fine', None, 'coarse')
- slab_ends: float32 [32, 1, 64, 64, 256], P('fine', None, 'coarse')
The draws below stay inside these ranges and needn't reach their ends.
All inputs are finite; a program needn't handle non-finite values.
Results may differ from the reference program's by a relative error of at most 0.014.
Values may be sent and summed in bfloat16 or wider, within the bound.
No kernel may reach another device: no remote copies, remote signals or barrier semaphores. Data moves between devices by JAX's collectives and lax.ppermute only.
A program may use at most 64 MiB of HBM per device.

```python
import math
import jax
import jax.numpy as jnp
from jax import lax

C = 256
LAYERS_DEV = 4
COLS = 64
BATCH = 1
SLABS = 32
LAYERS = 128
ROWS = 64
N_FINE = 32


def level_of(stream_key, shape, split, smallest, high):
    factor_of, own = 1.0, jax.random.fold_in(stream_key, 6)
    for axis_at, parts in split:
        heights = jnp.exp(jax.random.uniform(jax.random.fold_in(own, axis_at), (parts,), jnp.float32, smallest / len(split), high / len(split)))
        factor_of = factor_of * jnp.repeat(heights, shape[axis_at] // parts).reshape([-1 if axis == axis_at else 1 for axis in range(len(shape))])
    return factor_of


def scatter_about(stream_key, shape, deviation, reach, cuts=(), dtype=jnp.bfloat16):
    array = deviation * jax.random.normal(stream_key, shape, jnp.float32)
    if cuts:
        array = array * level_of(stream_key, shape, cuts, -0.22, 0.18)
    return jnp.clip(array, -reach, reach).astype(dtype)


def setup_inputs(seed: int = 0) -> dict:
    seeds = jax.random.split(jax.random.key(seed), 5)
    return {
        "start_states": scatter_about(seeds[0], (SLABS, BATCH, ROWS, COLS, C), 1.0, 6.0, ((0, 32), (2, 8)), jnp.float32),
        "weights": scatter_about(seeds[1], (LAYERS, 9, C, C), (9 * C) ** -0.5, 0.125, ((0, 32),)),
        "biases": scatter_about(seeds[2], (LAYERS, C), 0.5, 3.0, ((0, 32),), jnp.float32),
        "step_sizes": jnp.clip(jnp.exp(math.log(0.4) - 1.3862944 * jax.random.uniform(seeds[3], (LAYERS,), jnp.float32) ** level_of(seeds[3], (LAYERS,), ((0, 32),), -0.2, 0.2)), 0.1, 0.4),
    }


def conv_map(current_state, kernel):
    padded = jnp.pad(current_state.astype(jnp.bfloat16), ((0, 0), (1, 1), (1, 1), (0, 0)))
    row_count = current_state.shape[1]
    col_count = current_state.shape[2]
    channels = current_state.shape[3]
    tap_slices = [padded[:, row_shift:row_shift + row_count, col_shift:col_shift + col_count, :] for row_shift in range(3) for col_shift in range(3)]
    stacked = jnp.concatenate(tap_slices, axis=-1).reshape(-1, 9 * channels)
    product = jnp.dot(stacked, kernel.reshape(9 * channels, channels), preferred_element_type=jnp.float32)
    return product.reshape(current_state.shape)


def relax_slab(packed):
    current_state, slab_kernels, slab_biases, slab_steps = packed
    first_slope = jnp.zeros(current_state.shape, jnp.float32)
    for layer_index in range(LAYERS_DEV):
        slope_term = jnp.tanh(conv_map(current_state, slab_kernels[layer_index]) + slab_biases[layer_index])
        if layer_index == 0:
            first_slope = slope_term
        current_state = current_state + slab_steps[layer_index] * slope_term
    return current_state, first_slope


def reference(start_states, weights, biases, step_sizes):
    kernels = weights.reshape(N_FINE, LAYERS_DEV, 9, C, C)
    bias_rows = biases.reshape(N_FINE, LAYERS_DEV, C)
    step_rows = step_sizes.reshape(N_FINE, LAYERS_DEV)
    relaxed, first_slopes = lax.map(relax_slab, (start_states, kernels, bias_rows, step_rows))
    coarse_steps = jnp.sum(step_rows, axis=1)
    defects = relaxed - (start_states + coarse_steps[:, None, None, None, None] * first_slopes)

    def advance(carried, packed):
        kernel, bias_row, coarse_step, defect = packed
        following = carried + coarse_step * jnp.tanh(conv_map(carried, kernel) + bias_row) + defect
        return following, following

    ignored, chained = lax.scan(advance, start_states[0], (kernels[:-1, 0], bias_rows[:-1, 0], coarse_steps[:-1], defects[:-1]))
    corrected = jnp.concatenate([start_states[:1], chained], axis=0)
    slab_ends, unused = lax.map(relax_slab, (corrected, kernels, bias_rows, step_rows))
    return corrected, slab_ends
```

```python
import functools

import jax
import jax.numpy as jnp
from jax import lax
from jax.experimental import pallas as pl
from jax.experimental.pallas import tpu as pltpu
from jax.sharding import PartitionSpec as P

C = 256
COLS = 64
ROWS = 64
LAYERS = 4
OWN = 8
TILE = 4
GROUP = 4
PLANES = 8
TILES = ROWS // TILE
DEPTH = 7
WIDE = OWN + 2 * (DEPTH - LAYERS)
SENT = TILE + 2 * (GROUP - 1)
EXTRA = 16
BF16, F32 = jnp.bfloat16, jnp.float32
AXES = ("fine", "coarse")
VMEM = pl.BlockSpec(memory_space=pltpu.VMEM)
SMEM = pl.BlockSpec(memory_space=pltpu.SMEM)


def cells(row, rows):
    return pl.ds(row * COLS, rows * COLS)


def spread(wide, slot, row, values):
    col = lax.broadcasted_iota(jnp.int32, values.shape, 0)
    left = jnp.where(col == 0, 0.0, pltpu.roll(values, 1, 0))
    right = jnp.where(col == COLS - 1, 0.0, pltpu.roll(values, COLS - 1, 0))
    at = cells(row, 1)
    wide[slot, at, 0:C] = left.astype(BF16)
    wide[slot, at, C : 2 * C] = values.astype(BF16)
    wide[slot, at, 2 * C : 3 * C] = right.astype(BF16)


def convolve(wide, slot, kernel, row, rows):
    taps = [wide[slot, cells(row + a, rows), :] for a in range(3)]
    return jnp.dot(jnp.concatenate(taps, axis=1), kernel, preferred_element_type=F32)


def inside(row):
    return jnp.where((row >= 0) & (row < ROWS), 1.0, 0.0).astype(F32)


def chunks(rows, size):
    return [(row, min(size, rows - row)) for row in range(0, rows, size)]


def place():
    slab = lax.axis_index("fine")
    return slab // 4, (slab // 2) % 2, slab % 2, lax.axis_index("coarse")


def relax_rows(depth, first_row, read, weights, biases, steps, state, wide, visit):
    total = OWN + 2 * depth
    for row in range(total):
        values = read(row)
        state[cells(row, 1), :] = values
        spread(wide, 0, row, values)
    for layer in range(LAYERS):
        for start, rows in chunks(total - 2 * (layer + 1), 4):
            slope = jnp.tanh(
                convolve(wide, layer % 2, weights[layer], start, rows)
                + biases[layer : layer + 1, :]
            )
            for i in range(rows):
                row = start + i + layer + 1
                piece = slope[i * COLS : (i + 1) * COLS, :]
                values = state[cells(row, 1), :] + steps[layer] * piece
                if not depth <= row < depth + OWN:
                    values = values * inside(first_row + row - depth)
                state[cells(row, 1), :] = values
                if layer < LAYERS - 1:
                    spread(wide, (layer + 1) % 2, start + i, values)
                visit(layer, row, piece, values)


def split3(values):
    high = values.astype(BF16).astype(F32)
    rest = values - high
    middle = rest.astype(BF16).astype(F32)
    return [high, middle, rest - middle]


def prepare_kernel(initial, weights, to_below, to_above, kernel, sem):
    copy = pltpu.make_async_copy(weights.at[0], kernel, sem)
    copy.start()
    to_below[...] = initial[(OWN - DEPTH) * COLS :, :].astype(BF16)
    to_above[...] = initial[: DEPTH * COLS, :].astype(BF16)
    copy.wait()


def first_kernel(
    steps, up, own, down, weights, biases, same, other, relaxed, state, wide, gain
):
    plane, half, core, coarse = place()
    is_first = (plane == 0) & (half == 0) & (core == 0)
    total_step = steps[0] + steps[1] + steps[2] + steps[3]

    def read(row):
        if row < DEPTH:
            return up[cells(row, 1), :].astype(F32)
        if row < DEPTH + OWN:
            return own[cells(row - DEPTH, 1), :]
        return down[cells(row - DEPTH - OWN, 1), :].astype(F32)

    def visit(layer, row, slope, values):
        at = row - LAYERS
        if not 0 <= at < WIDE:
            return
        to = cells(at, 1)
        if layer == 0:
            gain[to, :] = (steps[0] - total_step) * slope
            return
        gained = gain[to, :] + steps[layer] * slope
        if layer == LAYERS - 1:
            gained = jnp.where(is_first, values, gained)
            if DEPTH <= row < DEPTH + OWN:
                relaxed[cells(row - DEPTH, 1), :] = values
        gain[to, :] = gained

    relax_rows(DEPTH, coarse * OWN, read, weights, biases, steps, state, wide, visit)
    pieces = split3(biases[0:1, :]) + split3(jnp.full((1, C), total_step, F32))
    pieces.append(jnp.zeros((EXTRA - len(pieces), C), F32))
    extra = jnp.concatenate(pieces, axis=0).astype(BF16)
    for ref, side in ((same, half), (other, 1 - half)):
        base = pl.multiple_of(side * (TILE * COLS), TILE * COLS)
        ref[0 : SENT * COLS, :] = gain[pl.ds(base, SENT * COLS), :].astype(BF16)
        ref[SENT * COLS :, :] = extra


def last_kernel(
    steps, initial, relaxed, mine, across, halo_a, halo_b, near, far, halo_c, halo_d,
    weights, biases, corrected, finished, state, wide,
):
    plane, half, core, coarse = place()
    is_first = (plane == 0) & (half == 0) & (core == 0)
    north, lower = core == 1, half == 1

    def read(row):
        at = cells(row % TILE, 1)
        a, b, c, d = (
            (halo_a, halo_b, halo_c, halo_d),
            (across, mine, far, near),
            (mine, across, near, far),
            (halo_b, halo_a, halo_d, halo_c),
        )[row // TILE]
        a, b, c, d = (ref[at, :].astype(F32) for ref in (a, b, c, d))
        values = jnp.where(north, jnp.where(lower, a, b), jnp.where(lower, c, d))
        if TILE <= row < TILE + OWN:
            to = cells(row - TILE, 1)
            corrected[to, :] = jnp.where(is_first, initial[to, :], values)
        return values

    def visit(layer, row, slope, values):
        if layer == LAYERS - 1:
            to = cells(row - LAYERS, 1)
            finished[to, :] = jnp.where(is_first, relaxed[to, :], values)

    relax_rows(LAYERS, coarse * OWN, read, weights, biases, steps, state, wide, visit)


def chain_kernel(turn, *refs):
    refs = list(refs)
    entering = None if turn == 0 else [refs.pop(0) for _ in range(3)]
    before = None if turn == 0 else [refs.pop(0) for _ in range(GROUP)]
    defects = [refs.pop(0) for _ in range(GROUP)]
    weights = refs.pop(0)
    following = None if turn == PLANES - 1 else refs.pop(0)
    passed = [refs.pop(0) for _ in range(GROUP)]
    state, wide, hold = refs
    plane, half, core, coarse = place()
    first_row = (coarse * 2 + half) * TILE - TILE
    active = (plane == turn) & (core == 1)

    def defect(step, at):
        a, b = defects[step][at, :].astype(F32), defects[step ^ 2][at, :].astype(F32)
        return jnp.where(half == 0, a, b)

    def keep(step, row, values):
        hold[step, cells(row - TILE, 1), :] = values.astype(BF16)

    @pl.when(jnp.logical_not(active))
    def _():
        for i in range(GROUP):
            passed[i][...] = jnp.zeros_like(passed[i]) if turn == 0 else before[i][...]
        if following is not None:
            following[...] = jnp.zeros_like(following)

    @pl.when(active)
    def _():
        if turn == 0:
            hold[0] = jnp.zeros(hold.shape[1:], BF16)
            for row in range(1, 1 + SENT):
                values = defect(0, cells(row - 1, 1))
                if TILE <= row < 2 * TILE:
                    keep(1, row, values)
                else:
                    values = values * inside(first_row + row)
                state[cells(row, 1), :] = values
                spread(wide, 1, row - 1, values)
        else:
            for row in range(3 * TILE):
                values = entering[row // TILE][cells(row % TILE, 1), :].astype(F32)
                state[cells(row, 1), :] = values
                spread(wide, 0, row, values)
                if TILE <= row < 2 * TILE:
                    keep(0, row, values)
        final = GROUP - 1 if turn == PLANES - 1 else GROUP
        for step in range(1 if turn == 0 else 0, final):
            extra = defect(step, pl.ds(SENT * COLS, EXTRA))
            bias = extra[0:1, :] + extra[1:2, :] + extra[2:3, :]
            scale = extra[3:4, :] + extra[4:5, :] + extra[5:6, :]
            kernel = weights[jnp.bitwise_xor(step, 2 * half)]
            for start, rows in chunks(3 * TILE - 2 * (step + 1), 2):
                slope = jnp.tanh(convolve(wide, step % 2, kernel, start, rows) + bias)
                for i in range(rows):
                    row = start + i + step + 1
                    piece = slope[i * COLS : (i + 1) * COLS, :]
                    values = state[cells(row, 1), :] + scale * piece
                    values = values + defect(step, cells(row - 1, 1))
                    if not TILE <= row < 2 * TILE:
                        values = values * inside(first_row + row)
                    elif step == GROUP - 1:
                        following[cells(row - TILE, 1), :] = values.astype(BF16)
                    else:
                        keep(step + 1, row, values)
                    if step < GROUP - 1:
                        state[cells(row, 1), :] = values
                        spread(wide, (step + 1) % 2, start + i, values)
        for i in range(GROUP):
            passed[i][...] = hold[jnp.bitwise_xor(i, 2 * half)]


def cost(row_products):
    flops = 2 * row_products * COLS * 9 * C * C
    return pl.CostEstimate(flops=flops, bytes_accessed=flops // 512, transcendentals=0)


def call(body, name, row_products, rows, outs, in_specs, more=()):
    return pl.pallas_call(
        body,
        name=name,
        out_shape=outs,
        in_specs=in_specs,
        out_specs=jax.tree.map(lambda _: VMEM, outs),
        scratch_shapes=[
            pltpu.VMEM((rows * COLS, C), F32),
            pltpu.VMEM((2, rows * COLS, 3 * C), BF16),
            *more,
        ],
        compiler_params=pltpu.CompilerParams(vmem_limit_bytes=16 * 2**20),
        cost_estimate=cost(row_products),
    )


def shape(rows, dtype=BF16):
    return jax.ShapeDtypeStruct((rows, C), dtype)


def device(plane, half, core, coarse):
    return ((plane * 2 + half) * 2 + core) * 8 + coarse


def tile_device(plane, tile):
    return device(plane, tile % 2, 1, tile // 2)


def beside(half, coarse, by):
    x = (2 * (coarse % 2) + half + by) % 4
    return x % 2, 2 * (coarse // 2) + x // 2


def within_plane(link):
    pairs = []
    for plane in range(PLANES):
        for half in range(2):
            for coarse in range(8):
                pairs.append(link(plane, half, coarse))
    return pairs


def local(start_states, weights, biases, step_sizes):
    initial = start_states.reshape(OWN * COLS, C)
    kernels = weights.reshape(LAYERS, 9 * C, C)
    downward = [(i, i + 1) for i in range(7)]
    upward = [(i + 1, i) for i in range(7)]

    to_below, to_above, kernel = pl.pallas_call(
        prepare_kernel,
        name="prepare",
        out_shape=(shape(DEPTH * COLS), shape(DEPTH * COLS), shape(9 * C)),
        in_specs=[VMEM, pl.BlockSpec(memory_space=pltpu.HBM)],
        out_specs=(VMEM, VMEM, VMEM),
        scratch_shapes=[pltpu.SemaphoreType.DMA(())],
        compiler_params=pltpu.CompilerParams(vmem_limit_bytes=8 * 2**20),
    )(initial, kernels)
    above = lax.ppermute(to_below, "coarse", downward)
    below = lax.ppermute(to_above, "coarse", upward)

    to_north = within_plane(lambda p, h, c: (device(p, h, 0, c), device(p, h, 1, c)))
    to_other_north = within_plane(
        lambda p, h, c: (device(p, h, 0, c), device(p, 1 - h, 1, c))
    )
    north_to_north = within_plane(
        lambda p, h, c: (device(p, h, 1, c), device(p, 1 - h, 1, c))
    )

    def from_right(p, h, c):
        half, coarse = beside(h, c, 1)
        return device(p, half, 0, coarse), device(p, h, 1, c)

    def from_left(p, h, c):
        half, coarse = beside(h, c, 1)
        return device(p, h, 1, c), device(p, half, 1, coarse)

    near_south = lax.ppermute(kernel, AXES, to_north)
    far_south = lax.ppermute(kernel, AXES, within_plane(from_right))
    far_north = lax.ppermute(kernel, AXES, within_plane(from_left))

    message = shape(SENT * COLS + EXTRA)
    same, other, relaxed = call(
        first_kernel,
        "first",
        68,
        OWN + 2 * DEPTH,
        (message, message, shape(OWN * COLS, F32)),
        [SMEM] + [VMEM] * 5,
        (pltpu.VMEM((WIDE * COLS, C), F32),),
    )(step_sizes, above, initial, below, kernels, biases)
    defects = [
        lax.ppermute(same, AXES, to_north),
        same,
        lax.ppermute(other, AXES, to_other_north),
        lax.ppermute(other, AXES, north_to_north),
    ]
    chain_kernels = jnp.stack([near_south, kernel, far_south, far_north])

    block = shape(TILE * COLS)
    entering, passed = [], []
    for turn in range(PLANES):
        last = turn == PLANES - 1
        outs = (block,) * (GROUP if last else GROUP + 1)
        operands = [*entering, *passed, *defects, chain_kernels]
        results = call(
            functools.partial(chain_kernel, turn),
            "chain",
            28,
            3 * TILE,
            outs,
            [VMEM] * len(operands),
            (pltpu.VMEM((GROUP, TILE * COLS, C), BF16),),
        )(*operands)
        passed = results[-GROUP:]
        if not last:
            own, up, down = (
                lax.ppermute(
                    results[0],
                    AXES,
                    [
                        (tile_device(turn, q), tile_device(turn + 1, q + by))
                        for q in range(TILES)
                        if 0 <= q + by < TILES
                    ],
                )
                for by in (0, 1, -1)
            )
            entering = [up, own, down]

    near_state, own_state, far_state, across_state = passed

    def halos(to_same, to_other_core):
        pairs = []
        for plane in range(PLANES):
            for coarse in range(8):
                if coarse > 0:
                    dest = device(plane, to_same, to_other_core, coarse)
                    pairs.append((device(plane, 1, 1, coarse - 1), dest))
                if coarse < 7:
                    dest = device(plane, 1 - to_same, to_other_core, coarse)
                    pairs.append((device(plane, 0, 1, coarse + 1), dest))
        return pairs

    across = lax.ppermute(across_state, AXES, north_to_north)
    halo_a = lax.ppermute(own_state, AXES, halos(1, 1))
    halo_b = lax.ppermute(across_state, AXES, halos(0, 1))
    near = lax.ppermute(near_state, AXES, [(b, a) for a, b in to_north])
    far = lax.ppermute(far_state, AXES, [(b, a) for a, b in to_other_north])
    halo_c = lax.ppermute(near_state, AXES, halos(1, 0))
    halo_d = lax.ppermute(far_state, AXES, halos(0, 0))
    result = shape(OWN * COLS, F32)
    corrected, finished = call(
        last_kernel,
        "last",
        44,
        OWN + 2 * LAYERS,
        (result, result),
        [SMEM] + [VMEM] * 12,
    )(
        step_sizes, initial, relaxed, own_state, across, halo_a, halo_b,
        near, far, halo_c, halo_d, kernels, biases,
    )
    return (
        corrected.reshape(start_states.shape),
        finished.reshape(start_states.shape),
    )


def solution(mesh):
    in_specs = (
        P("fine", None, "coarse", None, None),
        P("fine", None, None, None),
        P("fine", None),
        P("fine"),
    )
    out_specs = (P("fine", None, "coarse", None, None), P("fine", None, "coarse", None, None))
    return jax.shard_map(local, mesh=mesh, in_specs=in_specs, out_specs=out_specs, check_vma=False)
```

```python
import functools

import jax
import jax.numpy as jnp
from jax import lax
from jax.experimental import pallas as pl
from jax.experimental.pallas import tpu as pltpu
from jax.sharding import PartitionSpec as P


C = 256
COLS = 64
ROWS = 64
LAYERS = 4
OWN = 8
TILE = 4
GROUP = 4
PLANES = 8
TILES = ROWS // TILE
DEPTH = 7
WIDE = OWN + 2 * (DEPTH - LAYERS)
SENT = TILE + 2 * (GROUP - 1)
EXTRA = 16
BF16, F32 = jnp.bfloat16, jnp.float32
AXES = ("fine", "coarse")
VMEM = pl.BlockSpec(memory_space=pltpu.VMEM)
SMEM = pl.BlockSpec(memory_space=pltpu.SMEM)


def cells(row, rows):
    return pl.ds(row * COLS, rows * COLS)


def spread(wide, slot, row, values):
    col = lax.broadcasted_iota(jnp.int32, values.shape, 0)
    left = jnp.where(col == 0, 0.0, pltpu.roll(values, 1, 0))
    right = jnp.where(col == COLS - 1, 0.0, pltpu.roll(values, COLS - 1, 0))
    at = cells(row, 1)
    wide[slot, at, 0:C] = left.astype(BF16)
    wide[slot, at, C : 2 * C] = values.astype(BF16)
    wide[slot, at, 2 * C : 3 * C] = right.astype(BF16)


def convolve(wide, slot, kernel, row, rows):
    taps = [wide[slot, cells(row + a, rows), :] for a in range(3)]
    return jnp.dot(jnp.concatenate(taps, axis=1), kernel, preferred_element_type=F32)


def inside(row):
    return jnp.where((row >= 0) & (row < ROWS), 1.0, 0.0).astype(F32)


def chunks(rows, size):
    return [(row, min(size, rows - row)) for row in range(0, rows, size)]


def place():
    slab = lax.axis_index("fine")
    return slab // 4, (slab // 2) % 2, slab % 2, lax.axis_index("coarse")


def relax_rows(depth, first_row, read, weights, biases, steps, state, wide, visit):
    total = OWN + 2 * depth
    for row in range(total):
        values = read(row)
        state[cells(row, 1), :] = values
        spread(wide, 0, row, values)
    for layer in range(LAYERS):
        for start, rows in chunks(total - 2 * (layer + 1), 4):
            slope = jnp.tanh(
                convolve(wide, layer % 2, weights[layer], start, rows)
                + biases[layer : layer + 1, :]
            )
            for i in range(rows):
                row = start + i + layer + 1
                piece = slope[i * COLS : (i + 1) * COLS, :]
                values = state[cells(row, 1), :] + steps[layer] * piece
                if not depth <= row < depth + OWN:
                    values = values * inside(first_row + row - depth)
                state[cells(row, 1), :] = values
                if layer < LAYERS - 1:
                    spread(wide, (layer + 1) % 2, start + i, values)
                visit(layer, row, piece, values)


def split3(values):
    high = values.astype(BF16).astype(F32)
    rest = values - high
    middle = rest.astype(BF16).astype(F32)
    return [high, middle, rest - middle]


def prepare_kernel(initial, to_below, to_above):
    to_below[...] = initial[(OWN - DEPTH) * COLS :, :].astype(BF16)
    to_above[...] = initial[: DEPTH * COLS, :].astype(BF16)


def pick_kernel(weights, kernel):
    kernel[...] = weights[0]


def first_kernel(
    steps, up, own, down, weights, biases, same, other, relaxed, state, wide, gain
):
    plane, half, core, coarse = place()
    is_first = (plane == 0) & (half == 0) & (core == 0)
    total_step = steps[0] + steps[1] + steps[2] + steps[3]

    def read(row):
        if row < DEPTH:
            return up[cells(row, 1), :].astype(F32)
        if row < DEPTH + OWN:
            return own[cells(row - DEPTH, 1), :]
        return down[cells(row - DEPTH - OWN, 1), :].astype(F32)

    def visit(layer, row, slope, values):
        at = row - LAYERS
        if not 0 <= at < WIDE:
            return
        to = cells(at, 1)
        if layer == 0:
            gain[to, :] = (steps[0] - total_step) * slope
            return
        gained = gain[to, :] + steps[layer] * slope
        if layer == LAYERS - 1:
            gained = jnp.where(is_first, values, gained)
            if DEPTH <= row < DEPTH + OWN:
                relaxed[cells(row - DEPTH, 1), :] = values
        gain[to, :] = gained

    relax_rows(DEPTH, coarse * OWN, read, weights, biases, steps, state, wide, visit)
    pieces = split3(biases[0:1, :]) + split3(jnp.full((1, C), total_step, F32))
    pieces.append(jnp.zeros((EXTRA - len(pieces), C), F32))
    extra = jnp.concatenate(pieces, axis=0).astype(BF16)
    for ref, side in ((same, half), (other, 1 - half)):
        base = pl.multiple_of(side * (TILE * COLS), TILE * COLS)
        ref[0 : SENT * COLS, :] = gain[pl.ds(base, SENT * COLS), :].astype(BF16)
        ref[SENT * COLS :, :] = extra


def last_kernel(
    steps, initial, relaxed, mine, across, halo_a, halo_b, near, far, halo_c, halo_d,
    weights, biases, corrected, finished, state, wide,
):
    plane, half, core, coarse = place()
    is_first = (plane == 0) & (half == 0) & (core == 0)
    north, lower = core == 1, half == 1

    def read(row):
        at = cells(row % TILE, 1)
        a, b, c, d = (
            (halo_a, halo_b, halo_c, halo_d),
            (across, mine, far, near),
            (mine, across, near, far),
            (halo_b, halo_a, halo_d, halo_c),
        )[row // TILE]
        a, b, c, d = (ref[at, :].astype(F32) for ref in (a, b, c, d))
        values = jnp.where(north, jnp.where(lower, a, b), jnp.where(lower, c, d))
        if TILE <= row < TILE + OWN:
            to = cells(row - TILE, 1)
            corrected[to, :] = jnp.where(is_first, initial[to, :], values)
        return values

    def visit(layer, row, slope, values):
        if layer == LAYERS - 1:
            to = cells(row - LAYERS, 1)
            finished[to, :] = jnp.where(is_first, relaxed[to, :], values)

    relax_rows(LAYERS, coarse * OWN, read, weights, biases, steps, state, wide, visit)


def chain_kernel(turn, *refs):
    refs = list(refs)
    entering = None if turn == 0 else [refs.pop(0) for _ in range(3)]
    before = None if turn == 0 else [refs.pop(0) for _ in range(GROUP)]
    defects = [refs.pop(0) for _ in range(GROUP)]
    weights = refs.pop(0)
    following = None if turn == PLANES - 1 else refs.pop(0)
    passed = [refs.pop(0) for _ in range(GROUP)]
    state, wide, hold = refs
    plane, half, core, coarse = place()
    first_row = (coarse * 2 + half) * TILE - TILE
    active = (plane == turn) & (core == 1)

    def defect(step, at):
        a, b = defects[step][at, :].astype(F32), defects[step ^ 2][at, :].astype(F32)
        return jnp.where(half == 0, a, b)

    def keep(step, row, values):
        hold[step, cells(row - TILE, 1), :] = values.astype(BF16)

    @pl.when(jnp.logical_not(active))
    def _():
        for i in range(GROUP):
            passed[i][...] = jnp.zeros_like(passed[i]) if turn == 0 else before[i][...]
        if following is not None:
            following[...] = jnp.zeros_like(following)

    @pl.when(active)
    def _():
        if turn == 0:
            hold[0] = jnp.zeros(hold.shape[1:], BF16)
            for row in range(1, 1 + SENT):
                values = defect(0, cells(row - 1, 1))
                if TILE <= row < 2 * TILE:
                    keep(1, row, values)
                else:
                    values = values * inside(first_row + row)
                state[cells(row, 1), :] = values
                spread(wide, 1, row - 1, values)
        else:
            for row in range(3 * TILE):
                values = entering[row // TILE][cells(row % TILE, 1), :].astype(F32)
                state[cells(row, 1), :] = values
                spread(wide, 0, row, values)
                if TILE <= row < 2 * TILE:
                    keep(0, row, values)
        final = GROUP - 1 if turn == PLANES - 1 else GROUP
        for step in range(1 if turn == 0 else 0, final):
            extra = defect(step, pl.ds(SENT * COLS, EXTRA))
            bias = extra[0:1, :] + extra[1:2, :] + extra[2:3, :]
            scale = extra[3:4, :] + extra[4:5, :] + extra[5:6, :]
            kernel = weights[jnp.bitwise_xor(step, 2 * half)]
            for start, rows in chunks(3 * TILE - 2 * (step + 1), 2):
                slope = jnp.tanh(convolve(wide, step % 2, kernel, start, rows) + bias)
                for i in range(rows):
                    row = start + i + step + 1
                    piece = slope[i * COLS : (i + 1) * COLS, :]
                    values = state[cells(row, 1), :] + scale * piece
                    values = values + defect(step, cells(row - 1, 1))
                    if not TILE <= row < 2 * TILE:
                        values = values * inside(first_row + row)
                    elif step == GROUP - 1:
                        following[cells(row - TILE, 1), :] = values.astype(BF16)
                    else:
                        keep(step + 1, row, values)
                    if step < GROUP - 1:
                        state[cells(row, 1), :] = values
                        spread(wide, (step + 1) % 2, start + i, values)
        for i in range(GROUP):
            passed[i][...] = hold[jnp.bitwise_xor(i, 2 * half)]


def cost(row_products):
    flops = 2 * row_products * COLS * 9 * C * C
    return pl.CostEstimate(flops=flops, bytes_accessed=flops // 512, transcendentals=0)


def call(body, row_products, rows, outs, in_specs, more=()):
    return pl.pallas_call(
        body,
        out_shape=outs,
        in_specs=in_specs,
        out_specs=jax.tree.map(lambda _: VMEM, outs),
        scratch_shapes=[
            pltpu.VMEM((rows * COLS, C), F32),
            pltpu.VMEM((2, rows * COLS, 3 * C), BF16),
            *more,
        ],
        compiler_params=pltpu.CompilerParams(vmem_limit_bytes=16 * 2**20),
        cost_estimate=cost(row_products),
    )


def shape(rows, dtype=BF16):
    return jax.ShapeDtypeStruct((rows, C), dtype)


def device(plane, half, core, coarse):
    return ((plane * 2 + half) * 2 + core) * 8 + coarse


def tile_device(plane, tile):
    return device(plane, tile % 2, 1, tile // 2)


def beside(half, coarse, by):
    x = (2 * (coarse % 2) + half + by) % 4
    return x % 2, 2 * (coarse // 2) + x // 2


def within_plane(link):
    pairs = []
    for plane in range(PLANES):
        for half in range(2):
            for coarse in range(8):
                pairs.append(link(plane, half, coarse))
    return pairs


def local(start_states, weights, biases, step_sizes):
    initial = start_states.reshape(OWN * COLS, C)
    kernels = weights.reshape(LAYERS, 9 * C, C)
    downward = [(i, i + 1) for i in range(7)]
    upward = [(i + 1, i) for i in range(7)]

    to_below, to_above = pl.pallas_call(
        prepare_kernel,
        name="prepare",
        out_shape=(shape(DEPTH * COLS), shape(DEPTH * COLS)),
        in_specs=[VMEM],
        out_specs=(VMEM, VMEM),
        compiler_params=pltpu.CompilerParams(vmem_limit_bytes=8 * 2**20),
    )(initial)
    above = lax.ppermute(to_below, "coarse", downward)
    below = lax.ppermute(to_above, "coarse", upward)
    kernel = pl.pallas_call(
        pick_kernel,
        name="pick",
        out_shape=shape(9 * C),
        in_specs=[VMEM],
        out_specs=VMEM,
        compiler_params=pltpu.CompilerParams(vmem_limit_bytes=8 * 2**20),
    )(kernels)

    to_north = within_plane(lambda p, h, c: (device(p, h, 0, c), device(p, h, 1, c)))
    to_other_north = within_plane(
        lambda p, h, c: (device(p, h, 0, c), device(p, 1 - h, 1, c))
    )
    north_to_north = within_plane(
        lambda p, h, c: (device(p, h, 1, c), device(p, 1 - h, 1, c))
    )

    def from_right(p, h, c):
        half, coarse = beside(h, c, 1)
        return device(p, half, 0, coarse), device(p, h, 1, c)

    def from_left(p, h, c):
        half, coarse = beside(h, c, 1)
        return device(p, h, 1, c), device(p, half, 1, coarse)

    far_south = lax.ppermute(kernel, AXES, within_plane(from_right))
    far_north = lax.ppermute(kernel, AXES, within_plane(from_left))
    near_south = lax.ppermute(kernel, AXES, to_north)

    message = shape(SENT * COLS + EXTRA)
    same, other, relaxed = call(
        first_kernel,
        68,
        OWN + 2 * DEPTH,
        (message, message, shape(OWN * COLS, F32)),
        [SMEM] + [VMEM] * 5,
        (pltpu.VMEM((WIDE * COLS, C), F32),),
    )(step_sizes, above, initial, below, kernels, biases)
    other_south = lax.ppermute(other, AXES, to_other_north)
    other_north = lax.ppermute(other, AXES, north_to_north)
    same_south = lax.ppermute(same, AXES, to_north)
    defects = [same_south, same, other_south, other_north]
    chain_kernels = jnp.stack([near_south, kernel, far_south, far_north])

    block = shape(TILE * COLS)
    entering, passed = [], []
    for turn in range(PLANES):
        last = turn == PLANES - 1
        outs = (block,) * (GROUP if last else GROUP + 1)
        operands = [*entering, *passed, *defects, chain_kernels]
        results = call(
            functools.partial(chain_kernel, turn),
            28,
            3 * TILE,
            outs,
            [VMEM] * len(operands),
            (pltpu.VMEM((GROUP, TILE * COLS, C), BF16),),
        )(*operands)
        passed = results[-GROUP:]
        if not last:
            entering = []
            for by in (1, 0, -1):
                pairs = [
                    (tile_device(turn, q), tile_device(turn + 1, q + by))
                    for q in range(TILES)
                    if 0 <= q + by < TILES
                ]
                entering.append(lax.ppermute(results[0], AXES, pairs))

    near_state, own_state, far_state, across_state = passed

    def halos(to_same, to_other_core):
        pairs = []
        for plane in range(PLANES):
            for coarse in range(8):
                if coarse > 0:
                    dest = device(plane, to_same, to_other_core, coarse)
                    pairs.append((device(plane, 1, 1, coarse - 1), dest))
                if coarse < 7:
                    dest = device(plane, 1 - to_same, to_other_core, coarse)
                    pairs.append((device(plane, 0, 1, coarse + 1), dest))
        return pairs

    near = lax.ppermute(near_state, AXES, [(b, a) for a, b in to_north])
    far = lax.ppermute(far_state, AXES, [(b, a) for a, b in to_other_north])
    halo_c = lax.ppermute(near_state, AXES, halos(1, 0))
    halo_d = lax.ppermute(far_state, AXES, halos(0, 0))
    across = lax.ppermute(across_state, AXES, north_to_north)
    halo_a = lax.ppermute(own_state, AXES, halos(1, 1))
    halo_b = lax.ppermute(across_state, AXES, halos(0, 1))
    result = shape(OWN * COLS, F32)
    corrected, finished = call(
        last_kernel, 44, OWN + 2 * LAYERS, (result, result), [SMEM] + [VMEM] * 12
    )(
        step_sizes, initial, relaxed, own_state, across, halo_a, halo_b,
        near, far, halo_c, halo_d, kernels, biases,
    )
    return (
        corrected.reshape(start_states.shape),
        finished.reshape(start_states.shape),
    )


def solution(mesh):
    in_specs = (
        P("fine", None, "coarse", None, None),
        P("fine", None, None, None),
        P("fine", None),
        P("fine"),
    )
    out_specs = (P("fine", None, "coarse", None, None), P("fine", None, "coarse", None, None))
    return jax.shard_map(local, mesh=mesh, in_specs=in_specs, out_specs=out_specs, check_vma=False)
```

```python
import functools

import jax
import jax.numpy as jnp
from jax import lax
from jax.experimental import pallas as pl
from jax.experimental.pallas import tpu as pltpu
from jax.sharding import PartitionSpec as P


C = 256
COLS = 64
ROWS = 64
LAYERS = 4
OWN = 8
TILE = 4
GROUP = 4
PLANES = 8
TILES = ROWS // TILE
DEPTH = 7
WIDE = OWN + 2 * (DEPTH - LAYERS)
SENT = TILE + 2 * (GROUP - 1)
EXTRA = 16
BF16, F32 = jnp.bfloat16, jnp.float32
AXES = ("fine", "coarse")
VMEM = pl.BlockSpec(memory_space=pltpu.VMEM)
SMEM = pl.BlockSpec(memory_space=pltpu.SMEM)


def cells(row, rows):
    return pl.ds(row * COLS, rows * COLS)


def spread(wide, slot, row, values):
    col = lax.broadcasted_iota(jnp.int32, values.shape, 0)
    left = jnp.where(col == 0, 0.0, pltpu.roll(values, 1, 0))
    right = jnp.where(col == COLS - 1, 0.0, pltpu.roll(values, COLS - 1, 0))
    at = cells(row, 1)
    wide[slot, at, 0:C] = left.astype(BF16)
    wide[slot, at, C : 2 * C] = values.astype(BF16)
    wide[slot, at, 2 * C : 3 * C] = right.astype(BF16)


def convolve(wide, slot, kernel, row, rows):
    taps = [wide[slot, cells(row + a, rows), :] for a in range(3)]
    return jnp.dot(jnp.concatenate(taps, axis=1), kernel, preferred_element_type=F32)


def inside(row):
    return jnp.where((row >= 0) & (row < ROWS), 1.0, 0.0).astype(F32)


def chunks(rows, size):
    return [(row, min(size, rows - row)) for row in range(0, rows, size)]


def place():
    slab = lax.axis_index("fine")
    return slab // 4, (slab // 2) % 2, slab % 2, lax.axis_index("coarse")


def relax_rows(depth, first_row, read, weights, biases, steps, state, wide, visit):
    total = OWN + 2 * depth
    for row in range(total):
        values = read(row)
        state[cells(row, 1), :] = values
        spread(wide, 0, row, values)
    for layer in range(LAYERS):
        for start, rows in chunks(total - 2 * (layer + 1), 4):
            slope = jnp.tanh(
                convolve(wide, layer % 2, weights[layer], start, rows)
                + biases[layer : layer + 1, :]
            )
            for i in range(rows):
                row = start + i + layer + 1
                piece = slope[i * COLS : (i + 1) * COLS, :]
                values = state[cells(row, 1), :] + steps[layer] * piece
                if not depth <= row < depth + OWN:
                    values = values * inside(first_row + row - depth)
                state[cells(row, 1), :] = values
                if layer < LAYERS - 1:
                    spread(wide, (layer + 1) % 2, start + i, values)
                visit(layer, row, piece, values)


def split3(values):
    high = values.astype(BF16).astype(F32)
    rest = values - high
    middle = rest.astype(BF16).astype(F32)
    return [high, middle, rest - middle]


def prepare_kernel(initial, to_below, to_above):
    to_below[...] = initial[(OWN - DEPTH) * COLS :, :].astype(BF16)
    to_above[...] = initial[: DEPTH * COLS, :].astype(BF16)


def pick_kernel(weights, kernel):
    kernel[...] = weights[0]


def first_kernel(
    steps, up, own, down, weights, biases,
    same, other0, other1, other2, other3, relaxed, state, wide, gain,
):
    plane, half, core, coarse = place()
    is_first = (plane == 0) & (half == 0) & (core == 0)
    total_step = steps[0] + steps[1] + steps[2] + steps[3]

    def read(row):
        if row < DEPTH:
            return up[cells(row, 1), :].astype(F32)
        if row < DEPTH + OWN:
            return own[cells(row - DEPTH, 1), :]
        return down[cells(row - DEPTH - OWN, 1), :].astype(F32)

    def visit(layer, row, slope, values):
        at = row - LAYERS
        if not 0 <= at < WIDE:
            return
        to = cells(at, 1)
        if layer == 0:
            gain[to, :] = (steps[0] - total_step) * slope
            return
        gained = gain[to, :] + steps[layer] * slope
        if layer == LAYERS - 1:
            gained = jnp.where(is_first, values, gained)
            if DEPTH <= row < DEPTH + OWN:
                relaxed[cells(row - DEPTH, 1), :] = values
        gain[to, :] = gained

    relax_rows(DEPTH, coarse * OWN, read, weights, biases, steps, state, wide, visit)
    pieces = split3(biases[0:1, :]) + split3(jnp.full((1, C), total_step, F32))
    pieces.append(jnp.zeros((EXTRA - len(pieces), C), F32))
    extra = jnp.concatenate(pieces, axis=0).astype(BF16)
    sides = [(same, half, 0)]
    sides += [(ref, 1 - half, k) for k, ref in enumerate((other0, other1, other2, other3))]
    for ref, side, skip in sides:
        rows = SENT - 2 * skip
        base = pl.multiple_of(side * (TILE * COLS) + skip * COLS, COLS)
        ref[0 : rows * COLS, :] = gain[pl.ds(base, rows * COLS), :].astype(BF16)
        ref[rows * COLS :, :] = extra


def pack_kernel(own, across, arrived, mine, theirs):
    core = place()[2]

    @pl.when(core == 1)
    def _():
        mine[...] = own[...]
        theirs[...] = across[...]

    @pl.when(core == 0)
    def _():
        mine[...] = arrived[: TILE * COLS, :]
        theirs[...] = arrived[TILE * COLS :, :]


def last_kernel(
    steps, initial, relaxed, mine, across, halo_a, halo_b, weights, biases,
    corrected, finished, state, wide,
):
    plane, half, core, coarse = place()
    is_first = (plane == 0) & (half == 0) & (core == 0)

    def read(row):
        at = cells(row % TILE, 1)
        lower, upper = (
            (halo_a, halo_b),
            (across, mine),
            (mine, across),
            (halo_b, halo_a),
        )[row // TILE]
        values = jnp.where(half == 1, lower[at, :].astype(F32), upper[at, :].astype(F32))
        if TILE <= row < TILE + OWN:
            to = cells(row - TILE, 1)
            corrected[to, :] = jnp.where(is_first, initial[to, :], values)
        return values

    def visit(layer, row, slope, values):
        if layer == LAYERS - 1:
            to = cells(row - LAYERS, 1)
            finished[to, :] = jnp.where(is_first, relaxed[to, :], values)

    relax_rows(LAYERS, coarse * OWN, read, weights, biases, steps, state, wide, visit)


def chain_kernel(turn, *refs):
    refs = list(refs)
    entering = None if turn == 0 else [refs.pop(0) for _ in range(3)]
    before = None if turn == 0 else [refs.pop(0) for _ in range(GROUP)]
    near, own_defect, *others = [refs.pop(0) for _ in range(2 + GROUP)]
    sources = [(near, others[0]), (own_defect, others[1]), (others[2], near), (others[3], own_defect)]
    weights = refs.pop(0)
    following = None if turn == PLANES - 1 else refs.pop(0)
    if turn == PLANES - 1:
        to_south = refs.pop(0)
        near_part, far_part = to_south.at[: TILE * COLS, :], to_south.at[TILE * COLS :, :]
        own_part, across_part = refs.pop(0), refs.pop(0)
        passed = [near_part, own_part, far_part, across_part]
    else:
        passed = [refs.pop(0) for _ in range(GROUP)]
    state, wide, hold = refs
    plane, half, core, coarse = place()
    first_row = (coarse * 2 + half) * TILE - TILE
    active = (plane == turn) & (core == 1)

    def defect(step, row, rows, cut=1):
        picked = []
        for at_half in range(2):
            ref = sources[step][at_half]
            skip = step if any(ref is other for other in others) else 0
            start = (row - skip) * COLS if cut else (SENT - 2 * skip) * COLS
            picked.append(ref[pl.ds(start, rows), :].astype(F32))
        return jnp.where(half == 0, picked[0], picked[1])

    def keep(step, row, values):
        hold[step, cells(row - TILE, 1), :] = values.astype(BF16)

    @pl.when(jnp.logical_not(active))
    def _():
        for i in range(GROUP):
            passed[i][...] = jnp.zeros_like(passed[i]) if turn == 0 else before[i][...]
        if following is not None:
            following[...] = jnp.zeros_like(following)

    @pl.when(active)
    def _():
        if turn == 0:
            hold[0] = jnp.zeros(hold.shape[1:], BF16)
            for row in range(1, 1 + SENT):
                values = defect(0, row - 1, COLS)
                if TILE <= row < 2 * TILE:
                    keep(1, row, values)
                else:
                    values = values * inside(first_row + row)
                state[cells(row, 1), :] = values
                spread(wide, 1, row - 1, values)
        else:
            for row in range(3 * TILE):
                values = entering[row // TILE][cells(row % TILE, 1), :].astype(F32)
                state[cells(row, 1), :] = values
                spread(wide, 0, row, values)
                if TILE <= row < 2 * TILE:
                    keep(0, row, values)
        final = GROUP - 1 if turn == PLANES - 1 else GROUP
        for step in range(1 if turn == 0 else 0, final):
            extra = defect(step, 0, EXTRA, cut=0)
            bias = extra[0:1, :] + extra[1:2, :] + extra[2:3, :]
            scale = extra[3:4, :] + extra[4:5, :] + extra[5:6, :]
            kernel = weights[jnp.bitwise_xor(step, 2 * half)]
            for start, rows in chunks(3 * TILE - 2 * (step + 1), 2):
                slope = jnp.tanh(convolve(wide, step % 2, kernel, start, rows) + bias)
                for i in range(rows):
                    row = start + i + step + 1
                    piece = slope[i * COLS : (i + 1) * COLS, :]
                    values = state[cells(row, 1), :] + scale * piece
                    values = values + defect(step, row - 1, COLS)
                    if not TILE <= row < 2 * TILE:
                        values = values * inside(first_row + row)
                    elif step == GROUP - 1:
                        following[cells(row - TILE, 1), :] = values.astype(BF16)
                    else:
                        keep(step + 1, row, values)
                    if step < GROUP - 1:
                        state[cells(row, 1), :] = values
                        spread(wide, (step + 1) % 2, start + i, values)
        for i in range(GROUP):
            passed[i][...] = hold[jnp.bitwise_xor(i, 2 * half)]


def cost(row_products):
    flops = 2 * row_products * COLS * 9 * C * C
    return pl.CostEstimate(flops=flops, bytes_accessed=flops // 512, transcendentals=0)


def call(body, row_products, rows, outs, in_specs, more=()):
    return pl.pallas_call(
        body,
        out_shape=outs,
        in_specs=in_specs,
        out_specs=jax.tree.map(lambda _: VMEM, outs),
        scratch_shapes=[
            pltpu.VMEM((rows * COLS, C), F32),
            pltpu.VMEM((2, rows * COLS, 3 * C), BF16),
            *more,
        ],
        compiler_params=pltpu.CompilerParams(vmem_limit_bytes=16 * 2**20),
        cost_estimate=cost(row_products),
    )


def shape(rows, dtype=BF16):
    return jax.ShapeDtypeStruct((rows, C), dtype)


def device(plane, half, core, coarse):
    return ((plane * 2 + half) * 2 + core) * 8 + coarse


def tile_device(plane, tile):
    return device(plane, tile % 2, 1, tile // 2)


def beside(half, coarse, by):
    x = (2 * (coarse % 2) + half + by) % 4
    return x % 2, 2 * (coarse // 2) + x // 2


def within_plane(link):
    pairs = []
    for plane in range(PLANES):
        for half in range(2):
            for coarse in range(8):
                pairs.append(link(plane, half, coarse))
    return pairs


def local(start_states, weights, biases, step_sizes):
    initial = start_states.reshape(OWN * COLS, C)
    kernels = weights.reshape(LAYERS, 9 * C, C)
    downward = [(i, i + 1) for i in range(7)]
    upward = [(i + 1, i) for i in range(7)]

    to_below, to_above = pl.pallas_call(
        prepare_kernel,
        name="prepare",
        out_shape=(shape(DEPTH * COLS), shape(DEPTH * COLS)),
        in_specs=[VMEM],
        out_specs=(VMEM, VMEM),
        compiler_params=pltpu.CompilerParams(vmem_limit_bytes=8 * 2**20),
    )(initial)
    above = lax.ppermute(to_below, "coarse", downward)
    below = lax.ppermute(to_above, "coarse", upward)
    kernel = pl.pallas_call(
        pick_kernel,
        name="pick",
        out_shape=shape(9 * C),
        in_specs=[VMEM],
        out_specs=VMEM,
        compiler_params=pltpu.CompilerParams(vmem_limit_bytes=8 * 2**20),
    )(kernels)

    to_north = within_plane(lambda p, h, c: (device(p, h, 0, c), device(p, h, 1, c)))
    to_other_north = within_plane(
        lambda p, h, c: (device(p, h, 0, c), device(p, 1 - h, 1, c))
    )
    north_to_north = within_plane(
        lambda p, h, c: (device(p, h, 1, c), device(p, 1 - h, 1, c))
    )

    def from_next_pair(p, h, c):
        half, coarse = beside(h, c, 1 if h else -1)
        return device(p, half, 1, coarse), device(p, h, 1, c)

    unused = {device(0, 0, 0, c) for c in range(8)}
    pairs = [pair for pair in to_other_north if pair[0] not in unused]
    far_south = lax.ppermute(kernel, AXES, pairs)
    far_north = lax.ppermute(kernel, AXES, within_plane(from_next_pair))
    near_south = lax.ppermute(kernel, AXES, to_north)

    messages = [shape((SENT - 2 * k) * COLS + EXTRA) for k in (0, 0, 1, 2, 3)]
    same, *others, relaxed = call(
        first_kernel,
        68,
        OWN + 2 * DEPTH,
        (*messages, shape(OWN * COLS, F32)),
        [SMEM] + [VMEM] * 5,
        (pltpu.VMEM((WIDE * COLS, C), F32),),
    )(step_sizes, above, initial, below, kernels, biases)
    defects = []
    for k in range(GROUP):
        half, core = k // 2, k % 2
        pairs = [
            (device(p, half, core, c), device(p, 1 - half, 1, c))
            for p in range(PLANES)
            for c in range(8)
        ]
        defects.append(lax.ppermute(others[k], AXES, pairs))
    same_south = lax.ppermute(same, AXES, to_north)
    defects = [same_south, same, *defects]
    chain_kernels = jnp.stack([near_south, kernel, far_south, far_north])

    block = shape(TILE * COLS)
    entering, passed = [], []
    for turn in range(PLANES):
        last = turn == PLANES - 1
        outs = (shape(2 * TILE * COLS), block, block) if last else (block,) * (GROUP + 1)
        operands = [*entering, *passed, *defects, chain_kernels]
        results = call(
            functools.partial(chain_kernel, turn),
            28,
            3 * TILE,
            outs,
            [VMEM] * len(operands),
            (pltpu.VMEM((GROUP, TILE * COLS, C), BF16),),
        )(*operands)
        if not last:
            passed = results[-GROUP:]
            entering = []
            for by in (1, 0, -1):
                pairs = [
                    (tile_device(turn, q), tile_device(turn + 1, q + by))
                    for q in range(TILES)
                    if 0 <= q + by < TILES
                ]
                entering.append(lax.ppermute(results[0], AXES, pairs))

    to_south, own_state, across_state = results
    arrived = lax.ppermute(to_south, AXES, [(b, a) for a, b in to_north])
    mine, theirs = pl.pallas_call(
        pack_kernel,
        name="pack",
        out_shape=(block, block),
        in_specs=[VMEM] * 3,
        out_specs=(VMEM, VMEM),
        compiler_params=pltpu.CompilerParams(vmem_limit_bytes=8 * 2**20),
    )(own_state, across_state, arrived)

    def halos(half_of_lower):
        pairs = []
        for plane in range(PLANES):
            for core in range(2):
                for coarse in range(8):
                    if coarse > 0:
                        dest = device(plane, half_of_lower, core, coarse)
                        pairs.append((device(plane, 1, core, coarse - 1), dest))
                    if coarse < 7:
                        dest = device(plane, 1 - half_of_lower, core, coarse)
                        pairs.append((device(plane, 0, core, coarse + 1), dest))
        return pairs

    halo_a = lax.ppermute(mine, AXES, halos(1))
    halo_b = lax.ppermute(theirs, AXES, halos(0))
    swap = [
        (device(p, h, core, c), device(p, 1 - h, core, c))
        for p in range(PLANES)
        for h in range(2)
        for core in range(2)
        for c in range(8)
    ]
    across = lax.ppermute(theirs, AXES, swap)
    result = shape(OWN * COLS, F32)
    corrected, finished = call(
        last_kernel, 44, OWN + 2 * LAYERS, (result, result), [SMEM] + [VMEM] * 8
    )(step_sizes, initial, relaxed, mine, across, halo_a, halo_b, kernels, biases)
    return (
        corrected.reshape(start_states.shape),
        finished.reshape(start_states.shape),
    )


def solution(mesh):
    in_specs = (
        P("fine", None, "coarse", None, None),
        P("fine", None, None, None),
        P("fine", None),
        P("fine"),
    )
    out_specs = (P("fine", None, "coarse", None, None), P("fine", None, "coarse", None, None))
    return jax.shard_map(local, mesh=mesh, in_specs=in_specs, out_specs=out_specs, check_vma=False)
```

```python
import functools

import jax
import jax.numpy as jnp
from jax import lax
from jax.experimental import pallas as pl
from jax.experimental.pallas import tpu as pltpu
from jax.sharding import PartitionSpec as P


C = 256
COLS = 64
ROWS = 64
LAYERS = 4
OWN = 8
TILE = 4
GROUP = 4
PLANES = 8
TILES = ROWS // TILE
DEPTH = 7
WIDE = OWN + 2 * (DEPTH - LAYERS)
SENT = TILE + 2 * (GROUP - 1)
EXTRA = 16
BF16, F32 = jnp.bfloat16, jnp.float32
AXES = ("fine", "coarse")
VMEM = pl.BlockSpec(memory_space=pltpu.VMEM)
SMEM = pl.BlockSpec(memory_space=pltpu.SMEM)


def cells(row, rows):
    return pl.ds(row * COLS, rows * COLS)


def spread_at(wide, slot, at, values):
    col = lax.broadcasted_iota(jnp.int32, values.shape, 0)
    left = jnp.where(col == 0, 0.0, pltpu.roll(values, 1, 0))
    right = jnp.where(col == COLS - 1, 0.0, pltpu.roll(values, COLS - 1, 0))
    wide[slot, at, 0:C] = left.astype(BF16)
    wide[slot, at, C : 2 * C] = values.astype(BF16)
    wide[slot, at, 2 * C : 3 * C] = right.astype(BF16)


def spread(wide, slot, row, values):
    spread_at(wide, slot, cells(row, 1), values)


def convolve(wide, slot, kernel, row, rows):
    taps = [wide[slot, cells(row + a, rows), :] for a in range(3)]
    return jnp.dot(jnp.concatenate(taps, axis=1), kernel, preferred_element_type=F32)


def inside(row):
    return jnp.where((row >= 0) & (row < ROWS), 1.0, 0.0).astype(F32)


def chunks(rows, size):
    return [(row, min(size, rows - row)) for row in range(0, rows, size)]


def place():
    slab = lax.axis_index("fine")
    return slab // 4, (slab // 2) % 2, slab % 2, lax.axis_index("coarse")


def relax_rows(depth, first_row, read, weights, biases, steps, state, wide, visit):
    total = OWN + 2 * depth
    for row in range(total):
        values = read(row)
        state[cells(row, 1), :] = values
        spread(wide, 0, row, values)
    for layer in range(LAYERS):
        for start, rows in chunks(total - 2 * (layer + 1), 4):
            slope = jnp.tanh(
                convolve(wide, layer % 2, weights[layer], start, rows)
                + biases[layer : layer + 1, :]
            )
            for i in range(rows):
                row = start + i + layer + 1
                piece = slope[i * COLS : (i + 1) * COLS, :]
                values = state[cells(row, 1), :] + steps[layer] * piece
                if not depth <= row < depth + OWN:
                    values = values * inside(first_row + row - depth)
                state[cells(row, 1), :] = values
                if layer < LAYERS - 1:
                    spread(wide, (layer + 1) % 2, start + i, values)
                visit(layer, row, piece, values)


def split3(values):
    high = values.astype(BF16).astype(F32)
    rest = values - high
    middle = rest.astype(BF16).astype(F32)
    return [high, middle, rest - middle]


def prepare_kernel(initial, to_below, to_above):
    to_below[...] = initial[(OWN - DEPTH) * COLS :, :].astype(BF16)
    to_above[...] = initial[: DEPTH * COLS, :].astype(BF16)


def pick_kernel(weights, kernel, sem):
    copy = pltpu.make_async_copy(weights.at[0], kernel, sem)
    copy.start()
    copy.wait()


def first_kernel(
    steps, up, own, down, weights, biases,
    same, other0, other1, relaxed, state, wide, gain,
):
    plane, half, core, coarse = place()
    is_first = (plane == 0) & (half == 0) & (core == 0)
    total_step = steps[0] + steps[1] + steps[2] + steps[3]

    def read(row):
        if row < DEPTH:
            return up[cells(row, 1), :].astype(F32)
        if row < DEPTH + OWN:
            return own[cells(row - DEPTH, 1), :]
        return down[cells(row - DEPTH - OWN, 1), :].astype(F32)

    def visit(layer, row, slope, values):
        at = row - LAYERS
        if not 0 <= at < WIDE:
            return
        to = cells(at, 1)
        if layer == 0:
            gain[to, :] = (steps[0] - total_step) * slope
            return
        gained = gain[to, :] + steps[layer] * slope
        if layer == LAYERS - 1:
            gained = jnp.where(is_first, values, gained)
            if DEPTH <= row < DEPTH + OWN:
                relaxed[cells(row - DEPTH, 1), :] = values
        gain[to, :] = gained

    relax_rows(DEPTH, coarse * OWN, read, weights, biases, steps, state, wide, visit)
    pieces = split3(biases[0:1, :]) + split3(jnp.full((1, C), total_step, F32))
    pieces.append(jnp.zeros((EXTRA - len(pieces), C), F32))
    extra = jnp.concatenate(pieces, axis=0).astype(BF16)
    sides = [(same, half, 0)]
    sides += [(ref, 1 - half, k) for k, ref in enumerate((other0, other1))]
    for ref, side, skip in sides:
        rows = SENT - 2 * skip
        base = pl.multiple_of(side * (TILE * COLS) + skip * COLS, COLS)
        ref[0 : rows * COLS, :] = gain[pl.ds(base, rows * COLS), :].astype(BF16)
        ref[rows * COLS :, :] = extra


def pack_kernel(own, across, arrived, mine, theirs):
    core = place()[2]

    @pl.when(core == 1)
    def _():
        mine[...] = own[...]
        theirs[...] = across[...]

    @pl.when(core == 0)
    def _():
        mine[...] = arrived[: TILE * COLS, :]
        theirs[...] = arrived[TILE * COLS :, :]


FRAME = OWN + 2 * LAYERS


class Frame:
    def __init__(self, state, wide, steps, weights, biases):
        self.half, self.coarse = place()[1], place()[3]
        self.state, self.wide = state, wide
        self.steps, self.weights, self.biases = steps, weights, biases

    def start(self, row, rows):
        return jnp.where(self.half == 1, row, FRAME - row - rows)

    def span(self, row, rows, shift=0):
        first = (self.start(row, rows) + shift) * COLS
        return pl.ds(pl.multiple_of(first, COLS), rows * COLS)

    def put(self, slot, row, rows, values):
        for i in range(rows):
            piece = values[i * COLS : (i + 1) * COLS, :]
            at = self.start(row, rows) + i
            to = pl.ds(pl.multiple_of(at * COLS, COLS), COLS)
            self.state[to, :] = piece
            if slot is not None:
                spread_at(self.wide, slot, to, piece)

    def layer(self, layer, row, rows, outside):
        taps = [self.wide[layer % 2, self.span(row, rows, a - 1), :] for a in range(3)]
        product = jnp.dot(
            jnp.concatenate(taps, axis=1), self.weights[layer], preferred_element_type=F32
        )
        slope = jnp.tanh(product + self.biases[layer : layer + 1, :])
        values = self.state[self.span(row, rows), :] + self.steps[layer] * slope
        if outside:
            masked = []
            for i in range(rows):
                at = self.coarse * OWN + self.start(row, rows) + i - LAYERS
                masked.append(values[i * COLS : (i + 1) * COLS, :] * inside(at))
            values = jnp.concatenate(masked, axis=0)
        self.put((layer + 1) % 2 if layer < LAYERS - 1 else None, row, rows, values)


def early_kernel(
    steps, initial, halo, across, mine, weights, biases, corrected, part, edge, state, wide
):
    plane, half, core, _ = place()
    is_first = (plane == 0) & (half == 0) & (core == 0)
    frame = Frame(state, wide, steps, weights, biases)
    for block, ref in enumerate((halo, across, mine)):
        values = ref[...].astype(F32)
        frame.put(0, block * TILE, TILE, values)
        if block > 0:
            to = frame.span(block * TILE, TILE, -LAYERS)
            corrected[to, :] = jnp.where(is_first, initial[to, :], values)
    for layer in range(LAYERS):
        edge[cells(2 * layer, 2), :] = state[frame.span(10 - layer, 2), :]
        for start, rows in chunks(10 - 2 * layer, 4):
            row = layer + 1 + start
            frame.layer(layer, row, rows, row < TILE)
    part[...] = state[frame.span(TILE, TILE), :]


def late_kernel(steps, relaxed, halo, edge, part, weights, biases, finished, state, wide):
    plane, half, core, _ = place()
    is_first = (plane == 0) & (half == 0) & (core == 0)
    frame = Frame(state, wide, steps, weights, biases)
    frame.put(0, 3 * TILE, TILE, halo[...].astype(F32))
    for layer in range(LAYERS):
        frame.put(layer % 2, 10 - layer, 2, edge[cells(2 * layer, 2), :])
        frame.layer(layer, 11 - layer, TILE, layer < LAYERS - 1)
    for row, values in ((TILE, part[...]), (2 * TILE, state[frame.span(2 * TILE, TILE), :])):
        to = frame.span(row, TILE, -LAYERS)
        finished[to, :] = jnp.where(is_first, relaxed[to, :], values)


def chain_kernel(turn, *refs):
    refs = list(refs)
    entering = None if turn == 0 else [refs.pop(0) for _ in range(3)]
    before = None if turn == 0 else [refs.pop(0) for _ in range(GROUP)]
    near, mine, south, north = [refs.pop(0) for _ in range(4)]
    sources = [(near, south), (mine, north), (south, near), (north, mine)]
    weights = refs.pop(0)
    following = None if turn == PLANES - 1 else refs.pop(0)
    if turn == PLANES - 1:
        to_south = refs.pop(0)
        near_part, far_part = to_south.at[: TILE * COLS, :], to_south.at[TILE * COLS :, :]
        own_part, across_part = refs.pop(0), refs.pop(0)
        passed = [near_part, own_part, far_part, across_part]
    else:
        passed = [refs.pop(0) for _ in range(GROUP)]
    state, wide, hold = refs
    plane, half, core, coarse = place()
    first_row = (coarse * 2 + half) * TILE - TILE
    active = (plane == turn) & (core == 1)

    def defect(step, row, rows, cut=1):
        picked = []
        for at_half in range(2):
            ref = sources[step][at_half]
            skip = 1 if ref is north else 0
            start = (row - skip) * COLS if cut else (SENT - 2 * skip) * COLS
            picked.append(ref[pl.ds(start, rows), :].astype(F32))
        return jnp.where(half == 0, picked[0], picked[1])

    def keep(step, row, values):
        hold[step, cells(row - TILE, 1), :] = values.astype(BF16)

    @pl.when(jnp.logical_not(active))
    def _():
        for i in range(GROUP):
            passed[i][...] = jnp.zeros_like(passed[i]) if turn == 0 else before[i][...]
        if following is not None:
            following[...] = jnp.zeros_like(following)

    @pl.when(active)
    def _():
        if turn == 0:
            hold[0] = jnp.zeros(hold.shape[1:], BF16)
            for row in range(1, 1 + SENT):
                values = defect(0, row - 1, COLS)
                if TILE <= row < 2 * TILE:
                    keep(1, row, values)
                else:
                    values = values * inside(first_row + row)
                state[cells(row, 1), :] = values
                spread(wide, 1, row - 1, values)
        else:
            for row in range(3 * TILE):
                values = entering[row // TILE][cells(row % TILE, 1), :].astype(F32)
                state[cells(row, 1), :] = values
                spread(wide, 0, row, values)
                if TILE <= row < 2 * TILE:
                    keep(0, row, values)
        final = GROUP - 1 if turn == PLANES - 1 else GROUP
        for step in range(1 if turn == 0 else 0, final):
            extra = defect(step, 0, EXTRA, cut=0)
            bias = extra[0:1, :] + extra[1:2, :] + extra[2:3, :]
            scale = extra[3:4, :] + extra[4:5, :] + extra[5:6, :]
            kernel = weights[jnp.bitwise_xor(step, 2 * half)]
            for start, rows in chunks(3 * TILE - 2 * (step + 1), 2):
                slope = jnp.tanh(convolve(wide, step % 2, kernel, start, rows) + bias)
                for i in range(rows):
                    row = start + i + step + 1
                    piece = slope[i * COLS : (i + 1) * COLS, :]
                    values = state[cells(row, 1), :] + scale * piece
                    values = values + defect(step, row - 1, COLS)
                    if not TILE <= row < 2 * TILE:
                        values = values * inside(first_row + row)
                    elif step == GROUP - 1:
                        following[cells(row - TILE, 1), :] = values.astype(BF16)
                    else:
                        keep(step + 1, row, values)
                    if step < GROUP - 1:
                        state[cells(row, 1), :] = values
                        spread(wide, (step + 1) % 2, start + i, values)
        for i in range(GROUP):
            passed[i][...] = hold[jnp.bitwise_xor(i, 2 * half)]


def cost(row_products):
    flops = 2 * row_products * COLS * 9 * C * C
    return pl.CostEstimate(flops=flops, bytes_accessed=flops // 512, transcendentals=0)


def call(body, row_products, rows, outs, in_specs, more=()):
    return pl.pallas_call(
        body,
        out_shape=outs,
        in_specs=in_specs,
        out_specs=jax.tree.map(lambda _: VMEM, outs),
        scratch_shapes=[
            pltpu.VMEM((rows * COLS, C), F32),
            pltpu.VMEM((2, rows * COLS, 3 * C), BF16),
            *more,
        ],
        compiler_params=pltpu.CompilerParams(vmem_limit_bytes=16 * 2**20),
        cost_estimate=cost(row_products),
    )


def shape(rows, dtype=BF16):
    return jax.ShapeDtypeStruct((rows, C), dtype)


def device(plane, half, core, coarse):
    return ((plane * 2 + half) * 2 + core) * 8 + coarse


def tile_device(plane, tile):
    return device(plane, tile % 2, 1, tile // 2)


def beside(half, coarse, by):
    x = (2 * (coarse % 2) + half + by) % 4
    return x % 2, 2 * (coarse // 2) + x // 2


def within_plane(link):
    pairs = []
    for plane in range(PLANES):
        for half in range(2):
            for coarse in range(8):
                pairs.append(link(plane, half, coarse))
    return pairs


def local(start_states, weights, biases, step_sizes):
    initial = start_states.reshape(OWN * COLS, C)
    kernels = weights.reshape(LAYERS, 9 * C, C)
    downward = [(i, i + 1) for i in range(7)]
    upward = [(i + 1, i) for i in range(7)]

    to_below, to_above = pl.pallas_call(
        prepare_kernel,
        name="prepare",
        out_shape=(shape(DEPTH * COLS), shape(DEPTH * COLS)),
        in_specs=[VMEM],
        out_specs=(VMEM, VMEM),
        compiler_params=pltpu.CompilerParams(vmem_limit_bytes=8 * 2**20),
    )(initial)
    above = lax.ppermute(to_below, "coarse", downward)
    below = lax.ppermute(to_above, "coarse", upward)
    kernel = pl.pallas_call(
        pick_kernel,
        name="pick",
        out_shape=shape(9 * C),
        in_specs=[pl.BlockSpec(memory_space=pltpu.HBM)],
        out_specs=VMEM,
        scratch_shapes=[pltpu.SemaphoreType.DMA(())],
        compiler_params=pltpu.CompilerParams(vmem_limit_bytes=50 * 2**20),
    )(kernels)

    to_north = within_plane(lambda p, h, c: (device(p, h, 0, c), device(p, h, 1, c)))
    to_other_north = within_plane(
        lambda p, h, c: (device(p, h, 0, c), device(p, 1 - h, 1, c))
    )
    north_to_north = within_plane(
        lambda p, h, c: (device(p, h, 1, c), device(p, 1 - h, 1, c))
    )

    def from_next_pair(p, h, c):
        half, coarse = beside(h, c, 1 if h else -1)
        return device(p, half, 1, coarse), device(p, h, 1, c)

    unused = {device(0, 0, 0, c) for c in range(8)}
    pairs = [pair for pair in to_other_north if pair[0] not in unused]
    far_south = lax.ppermute(kernel, AXES, pairs)
    far_north = lax.ppermute(kernel, AXES, within_plane(from_next_pair))
    near_south = lax.ppermute(kernel, AXES, to_north)

    messages = [shape((SENT - 2 * k) * COLS + EXTRA) for k in (0, 0, 1)]
    same, *others, relaxed = call(
        first_kernel,
        68,
        OWN + 2 * DEPTH,
        (*messages, shape(OWN * COLS, F32)),
        [SMEM] + [VMEM] * 5,
        (pltpu.VMEM((WIDE * COLS, C), F32),),
    )(step_sizes, above, initial, below, kernels, biases)

    def exchange(planes):
        def send(message, link):
            chosen = [pair for pair in link if pair[0] // device(1, 0, 0, 0) in planes]
            return lax.ppermute(message, AXES, chosen)

        other_south = send(others[0], to_other_north)
        other_north = send(others[1], north_to_north)
        return [send(same, to_north), same, other_south, other_north]

    early = exchange(range(1))
    late = exchange(range(1, PLANES))
    chain_kernels = jnp.stack([near_south, kernel, far_south, far_north])

    block = shape(TILE * COLS)
    entering, passed = [], []
    for turn in range(PLANES):
        last = turn == PLANES - 1
        outs = (shape(2 * TILE * COLS), block, block) if last else (block,) * (GROUP + 1)
        defects = late if turn else early
        operands = [*entering, *passed, *defects, chain_kernels]
        results = call(
            functools.partial(chain_kernel, turn),
            28,
            3 * TILE,
            outs,
            [VMEM] * len(operands),
            (pltpu.VMEM((GROUP, TILE * COLS, C), BF16),),
        )(*operands)
        if not last:
            passed = results[-GROUP:]
            entering = []
            for by in (1, 0, -1):
                pairs = [
                    (tile_device(turn, q), tile_device(turn + 1, q + by))
                    for q in range(TILES)
                    if 0 <= q + by < TILES
                ]
                entering.append(lax.ppermute(results[0], AXES, pairs))

    to_south, own_state, across_state = results
    arrived = lax.ppermute(to_south, AXES, [(b, a) for a, b in to_north])
    mine, theirs = pl.pallas_call(
        pack_kernel,
        name="pack",
        out_shape=(block, block),
        in_specs=[VMEM] * 3,
        out_specs=(VMEM, VMEM),
        compiler_params=pltpu.CompilerParams(vmem_limit_bytes=8 * 2**20),
    )(own_state, across_state, arrived)

    def halos(half_of_lower):
        pairs = []
        for plane in range(PLANES):
            for core in range(2):
                for coarse in range(8):
                    if coarse > 0:
                        dest = device(plane, half_of_lower, core, coarse)
                        pairs.append((device(plane, 1, core, coarse - 1), dest))
                    if coarse < 7:
                        dest = device(plane, 1 - half_of_lower, core, coarse)
                        pairs.append((device(plane, 0, core, coarse + 1), dest))
        return pairs

    halo_a = lax.ppermute(mine, AXES, halos(1))
    halo_b = lax.ppermute(theirs, AXES, halos(0))
    swap = [
        (device(p, h, core, c), device(p, 1 - h, core, c))
        for p in range(PLANES)
        for h in range(2)
        for core in range(2)
        for c in range(8)
    ]
    across = lax.ppermute(theirs, AXES, swap)
    result = shape(OWN * COLS, F32)
    corrected, part, edge = call(
        early_kernel,
        28,
        FRAME,
        (result, shape(TILE * COLS, F32), shape(2 * LAYERS * COLS, F32)),
        [SMEM] + [VMEM] * 6,
    )(step_sizes, initial, halo_a, across, mine, kernels, biases)
    finished = call(late_kernel, 16, FRAME, result, [SMEM] + [VMEM] * 6)(
        step_sizes, relaxed, halo_b, edge, part, kernels, biases
    )
    return (
        corrected.reshape(start_states.shape),
        finished.reshape(start_states.shape),
    )


def solution(mesh):
    in_specs = (
        P("fine", None, "coarse", None, None),
        P("fine", None, None, None),
        P("fine", None),
        P("fine"),
    )
    out_specs = (P("fine", None, "coarse", None, None), P("fine", None, "coarse", None, None))
    return jax.shard_map(local, mesh=mesh, in_specs=in_specs, out_specs=out_specs, check_vma=False)
```

```python
import functools

import jax
import jax.numpy as jnp
from jax import lax
from jax.experimental import pallas as pl
from jax.experimental.pallas import tpu as pltpu
from jax.sharding import PartitionSpec as P


C = 256
COLS = 64
ROWS = 64
LAYERS = 4
OWN = 8
TILE = 4
GROUP = 4
PLANES = 8
TILES = ROWS // TILE
DEPTH = 7
WIDE = OWN + 2 * (DEPTH - LAYERS)
SENT = TILE + 2 * (GROUP - 1)
EXTRA = 16
BF16, F32 = jnp.bfloat16, jnp.float32
AXES = ("fine", "coarse")
VMEM = pl.BlockSpec(memory_space=pltpu.VMEM)
SMEM = pl.BlockSpec(memory_space=pltpu.SMEM)


def cells(row, rows):
    return pl.ds(row * COLS, rows * COLS)


def spread(wide, slot, row, values):
    col = lax.broadcasted_iota(jnp.int32, values.shape, 0)
    left = jnp.where(col == 0, 0.0, pltpu.roll(values, 1, 0))
    right = jnp.where(col == COLS - 1, 0.0, pltpu.roll(values, COLS - 1, 0))
    at = cells(row, 1)
    wide[slot, at, 0:C] = left.astype(BF16)
    wide[slot, at, C : 2 * C] = values.astype(BF16)
    wide[slot, at, 2 * C : 3 * C] = right.astype(BF16)


def convolve(wide, slot, kernel, row, rows):
    taps = [wide[slot, cells(row + a, rows), :] for a in range(3)]
    return jnp.dot(jnp.concatenate(taps, axis=1), kernel, preferred_element_type=F32)


def inside(row):
    return jnp.where((row >= 0) & (row < ROWS), 1.0, 0.0).astype(F32)


def chunks(rows, size):
    return [(row, min(size, rows - row)) for row in range(0, rows, size)]


def place():
    slab = lax.axis_index("fine")
    return slab // 4, (slab // 2) % 2, slab % 2, lax.axis_index("coarse")


def relax_rows(depth, first_row, read, weights, biases, steps, state, wide, visit):
    total = OWN + 2 * depth
    for row in range(total):
        values = read(row)
        state[cells(row, 1), :] = values
        spread(wide, 0, row, values)
    for layer in range(LAYERS):
        for start, rows in chunks(total - 2 * (layer + 1), 4):
            slope = jnp.tanh(
                convolve(wide, layer % 2, weights[layer], start, rows)
                + biases[layer : layer + 1, :]
            )
            for i in range(rows):
                row = start + i + layer + 1
                piece = slope[i * COLS : (i + 1) * COLS, :]
                values = state[cells(row, 1), :] + steps[layer] * piece
                if not depth <= row < depth + OWN:
                    values = values * inside(first_row + row - depth)
                state[cells(row, 1), :] = values
                if layer < LAYERS - 1:
                    spread(wide, (layer + 1) % 2, start + i, values)
                visit(layer, row, piece, values)


def split3(values):
    high = values.astype(BF16).astype(F32)
    rest = values - high
    middle = rest.astype(BF16).astype(F32)
    return [high, middle, rest - middle]


def prepare_kernel(initial, to_below, to_above):
    to_below[...] = initial[(OWN - DEPTH) * COLS :, :].astype(BF16)
    to_above[...] = initial[: DEPTH * COLS, :].astype(BF16)


def pick_kernel(weights, kernel, sem):
    copy = pltpu.make_async_copy(weights.at[0], kernel, sem)
    copy.start()
    copy.wait()


def first_kernel(
    steps, up, own, down, weights, biases,
    same, other0, other1, relaxed, state, wide, gain,
):
    plane, half, core, coarse = place()
    is_first = (plane == 0) & (half == 0) & (core == 0)
    total_step = steps[0] + steps[1] + steps[2] + steps[3]

    def read(row):
        if row < DEPTH:
            return up[cells(row, 1), :].astype(F32)
        if row < DEPTH + OWN:
            return own[cells(row - DEPTH, 1), :]
        return down[cells(row - DEPTH - OWN, 1), :].astype(F32)

    def visit(layer, row, slope, values):
        at = row - LAYERS
        if not 0 <= at < WIDE:
            return
        to = cells(at, 1)
        if layer == 0:
            gain[to, :] = (steps[0] - total_step) * slope
            return
        gained = gain[to, :] + steps[layer] * slope
        if layer == LAYERS - 1:
            gained = jnp.where(is_first, values, gained)
            if DEPTH <= row < DEPTH + OWN:
                relaxed[cells(row - DEPTH, 1), :] = values
        gain[to, :] = gained

    relax_rows(DEPTH, coarse * OWN, read, weights, biases, steps, state, wide, visit)
    pieces = split3(biases[0:1, :]) + split3(jnp.full((1, C), total_step, F32))
    pieces.append(jnp.zeros((EXTRA - len(pieces), C), F32))
    extra = jnp.concatenate(pieces, axis=0).astype(BF16)
    sides = [(same, half, 0)]
    sides += [(ref, 1 - half, k) for k, ref in enumerate((other0, other1))]
    for ref, side, skip in sides:
        rows = SENT - 2 * skip
        base = pl.multiple_of(side * (TILE * COLS) + skip * COLS, COLS)
        ref[0 : rows * COLS, :] = gain[pl.ds(base, rows * COLS), :].astype(BF16)
        ref[rows * COLS :, :] = extra


def pack_kernel(own, across, arrived, mine, theirs):
    core = place()[2]

    @pl.when(core == 1)
    def _():
        mine[...] = own[...]
        theirs[...] = across[...]

    @pl.when(core == 0)
    def _():
        mine[...] = arrived[: TILE * COLS, :]
        theirs[...] = arrived[TILE * COLS :, :]


def last_kernel(
    steps, initial, relaxed, mine, across, halo_a, halo_b, weights, biases,
    corrected, finished, state, wide,
):
    plane, half, core, coarse = place()
    is_first = (plane == 0) & (half == 0) & (core == 0)

    def read(row):
        at = cells(row % TILE, 1)
        lower, upper = (
            (halo_a, halo_b),
            (across, mine),
            (mine, across),
            (halo_b, halo_a),
        )[row // TILE]
        values = jnp.where(half == 1, lower[at, :].astype(F32), upper[at, :].astype(F32))
        if TILE <= row < TILE + OWN:
            to = cells(row - TILE, 1)
            corrected[to, :] = jnp.where(is_first, initial[to, :], values)
        return values

    def visit(layer, row, slope, values):
        if layer == LAYERS - 1:
            to = cells(row - LAYERS, 1)
            finished[to, :] = jnp.where(is_first, relaxed[to, :], values)

    relax_rows(LAYERS, coarse * OWN, read, weights, biases, steps, state, wide, visit)


def chain_kernel(turn, *refs):
    refs = list(refs)
    entering = None if turn == 0 else [refs.pop(0) for _ in range(3)]
    before = None if turn == 0 else [refs.pop(0) for _ in range(GROUP)]
    near, mine, south, north = [refs.pop(0) for _ in range(4)]
    sources = [(near, south), (mine, north), (south, near), (north, mine)]
    weights = refs.pop(0)
    following = None if turn == PLANES - 1 else refs.pop(0)
    if turn == PLANES - 1:
        to_south = refs.pop(0)
        near_part, far_part = to_south.at[: TILE * COLS, :], to_south.at[TILE * COLS :, :]
        own_part, across_part = refs.pop(0), refs.pop(0)
        passed = [near_part, own_part, far_part, across_part]
    else:
        passed = [refs.pop(0) for _ in range(GROUP)]
    state, wide, hold = refs
    plane, half, core, coarse = place()
    first_row = (coarse * 2 + half) * TILE - TILE
    active = (plane == turn) & (core == 1)

    def defect(step, row, rows, cut=1):
        picked = []
        for at_half in range(2):
            ref = sources[step][at_half]
            skip = 1 if ref is north else 0
            start = (row - skip) * COLS if cut else (SENT - 2 * skip) * COLS
            picked.append(ref[pl.ds(start, rows), :].astype(F32))
        return jnp.where(half == 0, picked[0], picked[1])

    def keep(step, row, values):
        hold[step, cells(row - TILE, 1), :] = values.astype(BF16)

    @pl.when(jnp.logical_not(active))
    def _():
        for i in range(GROUP):
            passed[i][...] = jnp.zeros_like(passed[i]) if turn == 0 else before[i][...]
        if following is not None:
            following[...] = jnp.zeros_like(following)

    @pl.when(active)
    def _():
        if turn == 0:
            hold[0] = jnp.zeros(hold.shape[1:], BF16)
            for row in range(1, 1 + SENT):
                values = defect(0, row - 1, COLS)
                if TILE <= row < 2 * TILE:
                    keep(1, row, values)
                else:
                    values = values * inside(first_row + row)
                state[cells(row, 1), :] = values
                spread(wide, 1, row - 1, values)
        else:
            for row in range(3 * TILE):
                values = entering[row // TILE][cells(row % TILE, 1), :].astype(F32)
                state[cells(row, 1), :] = values
                spread(wide, 0, row, values)
                if TILE <= row < 2 * TILE:
                    keep(0, row, values)
        final = GROUP - 1 if turn == PLANES - 1 else GROUP
        for step in range(1 if turn == 0 else 0, final):
            extra = defect(step, 0, EXTRA, cut=0)
            bias = extra[0:1, :] + extra[1:2, :] + extra[2:3, :]
            scale = extra[3:4, :] + extra[4:5, :] + extra[5:6, :]
            kernel = weights[jnp.bitwise_xor(step, 2 * half)]
            spare = 1 if turn == PLANES - 1 else 0
            for start, rows in chunks(3 * TILE - 2 * (step + 1 + spare), 2):
                start += spare
                slope = jnp.tanh(convolve(wide, step % 2, kernel, start, rows) + bias)
                for i in range(rows):
                    row = start + i + step + 1
                    piece = slope[i * COLS : (i + 1) * COLS, :]
                    values = state[cells(row, 1), :] + scale * piece
                    values = values + defect(step, row - 1, COLS)
                    if not TILE <= row < 2 * TILE:
                        values = values * inside(first_row + row)
                    elif step == GROUP - 1:
                        following[cells(row - TILE, 1), :] = values.astype(BF16)
                    else:
                        keep(step + 1, row, values)
                    if step < GROUP - 1:
                        state[cells(row, 1), :] = values
                        spread(wide, (step + 1) % 2, start + i, values)
        for i in range(GROUP):
            passed[i][...] = hold[jnp.bitwise_xor(i, 2 * half)]


def cost(row_products):
    flops = 2 * row_products * COLS * 9 * C * C
    return pl.CostEstimate(flops=flops, bytes_accessed=flops // 512, transcendentals=0)


def call(body, row_products, rows, outs, in_specs, more=()):
    return pl.pallas_call(
        body,
        out_shape=outs,
        in_specs=in_specs,
        out_specs=jax.tree.map(lambda _: VMEM, outs),
        scratch_shapes=[
            pltpu.VMEM((rows * COLS, C), F32),
            pltpu.VMEM((2, rows * COLS, 3 * C), BF16),
            *more,
        ],
        compiler_params=pltpu.CompilerParams(vmem_limit_bytes=16 * 2**20),
        cost_estimate=cost(row_products),
    )


def shape(rows, dtype=BF16):
    return jax.ShapeDtypeStruct((rows, C), dtype)


def device(plane, half, core, coarse):
    return ((plane * 2 + half) * 2 + core) * 8 + coarse


def tile_device(plane, tile):
    return device(plane, tile % 2, 1, tile // 2)


def beside(half, coarse, by):
    x = (2 * (coarse % 2) + half + by) % 4
    return x % 2, 2 * (coarse // 2) + x // 2


def within_plane(link):
    pairs = []
    for plane in range(PLANES):
        for half in range(2):
            for coarse in range(8):
                pairs.append(link(plane, half, coarse))
    return pairs


def local(start_states, weights, biases, step_sizes):
    initial = start_states.reshape(OWN * COLS, C)
    kernels = weights.reshape(LAYERS, 9 * C, C)
    downward = [(i, i + 1) for i in range(7)]
    upward = [(i + 1, i) for i in range(7)]

    to_below, to_above = pl.pallas_call(
        prepare_kernel,
        name="prepare",
        out_shape=(shape(DEPTH * COLS), shape(DEPTH * COLS)),
        in_specs=[VMEM],
        out_specs=(VMEM, VMEM),
        compiler_params=pltpu.CompilerParams(vmem_limit_bytes=8 * 2**20),
    )(initial)
    above = lax.ppermute(to_below, "coarse", downward)
    below = lax.ppermute(to_above, "coarse", upward)
    kernel = pl.pallas_call(
        pick_kernel,
        name="pick",
        out_shape=shape(9 * C),
        in_specs=[pl.BlockSpec(memory_space=pltpu.HBM)],
        out_specs=VMEM,
        scratch_shapes=[pltpu.SemaphoreType.DMA(())],
        compiler_params=pltpu.CompilerParams(vmem_limit_bytes=50 * 2**20),
    )(kernels)

    to_north = within_plane(lambda p, h, c: (device(p, h, 0, c), device(p, h, 1, c)))
    to_other_north = within_plane(
        lambda p, h, c: (device(p, h, 0, c), device(p, 1 - h, 1, c))
    )
    north_to_north = within_plane(
        lambda p, h, c: (device(p, h, 1, c), device(p, 1 - h, 1, c))
    )

    def from_next_pair(p, h, c):
        half, coarse = beside(h, c, 1 if h else -1)
        return device(p, half, 1, coarse), device(p, h, 1, c)

    unused = {device(0, 0, 0, c) for c in range(8)}
    pairs = [pair for pair in to_other_north if pair[0] not in unused]
    far_south = lax.ppermute(kernel, AXES, pairs)
    far_north = lax.ppermute(kernel, AXES, within_plane(from_next_pair))
    near_south = lax.ppermute(kernel, AXES, to_north)

    messages = [shape((SENT - 2 * k) * COLS + EXTRA) for k in (0, 0, 1)]
    same, *others, relaxed = call(
        first_kernel,
        68,
        OWN + 2 * DEPTH,
        (*messages, shape(OWN * COLS, F32)),
        [SMEM] + [VMEM] * 5,
        (pltpu.VMEM((WIDE * COLS, C), F32),),
    )(step_sizes, above, initial, below, kernels, biases)

    def exchange(planes):
        def send(message, link):
            chosen = [pair for pair in link if pair[0] // device(1, 0, 0, 0) in planes]
            return lax.ppermute(message, AXES, chosen)

        other_south = send(others[0], to_other_north)
        other_north = send(others[1], north_to_north)
        return [send(same, to_north), same, other_south, other_north]

    early = exchange(range(1))
    late = exchange(range(1, PLANES))
    chain_kernels = jnp.stack([near_south, kernel, far_south, far_north])

    block = shape(TILE * COLS)
    entering, passed = [], []
    for turn in range(PLANES):
        last = turn == PLANES - 1
        outs = (shape(2 * TILE * COLS), block, block) if last else (block,) * (GROUP + 1)
        defects = late if turn else early
        operands = [*entering, *passed, *defects, chain_kernels]
        results = call(
            functools.partial(chain_kernel, turn),
            28,
            3 * TILE,
            outs,
            [VMEM] * len(operands),
            (pltpu.VMEM((GROUP, TILE * COLS, C), BF16),),
        )(*operands)
        if not last:
            passed = results[-GROUP:]
            entering = []
            for by in (1, 0, -1):
                pairs = [
                    (tile_device(turn, q), tile_device(turn + 1, q + by))
                    for q in range(TILES)
                    if 0 <= q + by < TILES
                ]
                entering.append(lax.ppermute(results[0], AXES, pairs))

    to_south, own_state, across_state = results
    arrived = lax.ppermute(to_south, AXES, [(b, a) for a, b in to_north])
    mine, theirs = pl.pallas_call(
        pack_kernel,
        name="pack",
        out_shape=(block, block),
        in_specs=[VMEM] * 3,
        out_specs=(VMEM, VMEM),
        compiler_params=pltpu.CompilerParams(vmem_limit_bytes=8 * 2**20),
    )(own_state, across_state, arrived)

    def halos(half_of_lower):
        pairs = []
        for plane in range(PLANES):
            for core in range(2):
                for coarse in range(8):
                    if coarse > 0:
                        dest = device(plane, half_of_lower, core, coarse)
                        pairs.append((device(plane, 1, core, coarse - 1), dest))
                    if coarse < 7:
                        dest = device(plane, 1 - half_of_lower, core, coarse)
                        pairs.append((device(plane, 0, core, coarse + 1), dest))
        return pairs

    halo_a = lax.ppermute(mine, AXES, halos(1))
    halo_b = lax.ppermute(theirs, AXES, halos(0))
    swap = [
        (device(p, h, core, c), device(p, 1 - h, core, c))
        for p in range(PLANES)
        for h in range(2)
        for core in range(2)
        for c in range(8)
    ]
    across = lax.ppermute(theirs, AXES, swap)
    result = shape(OWN * COLS, F32)
    corrected, finished = call(
        last_kernel, 44, OWN + 2 * LAYERS, (result, result), [SMEM] + [VMEM] * 8
    )(step_sizes, initial, relaxed, mine, across, halo_a, halo_b, kernels, biases)
    return (
        corrected.reshape(start_states.shape),
        finished.reshape(start_states.shape),
    )


def solution(mesh):
    in_specs = (
        P("fine", None, "coarse", None, None),
        P("fine", None, None, None),
        P("fine", None),
        P("fine"),
    )
    out_specs = (P("fine", None, "coarse", None, None), P("fine", None, "coarse", None, None))
    return jax.shard_map(local, mesh=mesh, in_specs=in_specs, out_specs=out_specs, check_vma=False)
```
